32 devices in a mesh: gx: 4 (over x, core), gy: 4 (over z), gz: 2 (over y).
Axes of the slice: x: 2, y: 2, z: 4, core: 2. Of those that a mesh axis runs over, the one named last changes fastest.
Arguments:
- points: float32 [16384, 768], P(('gx', 'gy', 'gz')), may hold values from -6 to 6
- assignment: int32 [16384], P(('gx', 'gy', 'gz')), may hold values from 0 to 32767, as said below
- sample_index: int32 [16384], P(('gx', 'gy', 'gz')), may hold values from 0 to 511
Outputs:
- means: float32 [32768, 768], P(('gx', 'gy', 'gz'))
- centroids: float32 [32768, 768], P(('gx', 'gy', 'gz'))
The draws below stay inside these ranges and needn't reach their ends.
Inputs may be any that keep to these rules, and one draw needn't show every extreme that they name: `assignment`: among the 512 points of one aligned block, at most 32 have a cluster in any one range of 1024 consecutive cluster numbers that starts at a multiple of 1024; in every block some range holds exactly 32.
All inputs are finite; a program needn't handle non-finite values.
Results may differ from the reference program's by a relative error of at most 0.00007.
Values sent between devices are 32-bit elements; how exact they have to be, the bound alone decides.
No kernel may reach another device: no remote copies, remote signals or barrier semaphores. Data moves between devices by JAX's collectives and lax.ppermute only.
A program may use at most 64 MiB of HBM per device.

```python
import jax
import jax.numpy as jnp
from jax import lax

D = 768
CL_DEV = 1024
PTS_DEV = 512
POINTS = 16384
CLUSTERS = 32768
CAP = 32
DEVICES = 32


def draw_assignment(key, part):
    slots_all = DEVICES * CAP

    def one_block(block_key):
        first, second, third, fourth = jax.random.split(block_key, 4)
        order = jax.random.permutation(first, slots_all)
        slot_ids = jnp.arange(slots_all, dtype=jnp.int32)
        rank_of = jnp.zeros((slots_all,), jnp.int32).at[order].set(slot_ids)
        heavy = jax.random.randint(second, (), 0, DEVICES)
        score = jnp.where(slot_ids // CAP == heavy, slot_ids - slots_all, rank_of)
        taken = jnp.argsort(score, stable=True)[:PTS_DEV]
        owner = jax.random.permutation(third, taken // CAP)
        inside = jax.random.randint(fourth, (PTS_DEV,), 0, CL_DEV)
        return owner * CL_DEV + inside
    keys = jax.random.split(jax.random.fold_in(key, 11), DEVICES)
    return jax.vmap(one_block)(keys).reshape(POINTS).astype(jnp.int32)


def touch_ends(drawn, key, least, largest):
    index_at = [jax.random.randint(jax.random.fold_in(key, axis), (), 0, length) for axis, length in enumerate(drawn.shape)]
    longest = drawn.shape.index(max(drawn.shape))
    beside = index_at[:longest] + [(index_at[longest] + 1) % drawn.shape[longest]] + index_at[longest + 1:]
    return drawn.at[tuple(index_at)].set(least).at[tuple(beside)].set(largest)


def shard_levels(own_key, dims, cuts, low, high):
    loudness, own = 1.0, jax.random.fold_in(own_key, 6)
    for axis_at, parts in cuts:
        draws = jnp.exp(jax.random.uniform(jax.random.fold_in(own, axis_at), (parts,), jnp.float32, low / len(cuts), high / len(cuts)))
        loudness = loudness * jnp.repeat(draws, dims[axis_at] // parts).reshape([-1 if axis == axis_at else 1 for axis in range(len(dims))])
    return loudness


def scatter_about(rng, dims, spread, most, pieces=(), held_as=jnp.bfloat16):
    values = jax.random.normal(rng, dims, jnp.float32) * spread
    if len(pieces) > 0:
        values = shard_levels(rng, dims, pieces, -0.22, 0.18) * values
    return jnp.clip(values, min=-most, max=most).astype(held_as)


def setup_inputs(seed: int = 0) -> dict:
    arg_keys = jax.random.split(jax.random.key(seed), 4)
    return {
        "points": scatter_about(arg_keys[0], (POINTS, D), 1.0, 6.0, ((0, 32),), jnp.float32),
        "assignment": draw_assignment(jax.random.fold_in(arg_keys[3], 71), 0),
        "sample_index": touch_ends(jax.random.randint(arg_keys[2], (POINTS,), 0, PTS_DEV), jax.random.fold_in(arg_keys[2], 1), 0, PTS_DEV - 1).astype(jnp.int32),
    }


def reference(points, assignment, sample_index):
    slots = jnp.arange(POINTS, dtype=jnp.int32)
    picked = slots // PTS_DEV * PTS_DEV + sample_index.astype(jnp.int32)
    weight = jax.ops.segment_sum(jnp.ones((POINTS,), points.dtype), picked, num_segments=POINTS)
    totals = jax.ops.segment_sum(points * weight[:, None], assignment, num_segments=CLUSTERS)
    tally = jax.ops.segment_sum(weight, assignment, num_segments=CLUSTERS)
    means = totals / jnp.maximum(tally, 1.0)[:, None]
    centroids = means / jnp.sqrt(lax.optimization_barrier(jnp.sum(means * means, axis=1, keepdims=True)) + 1e-06)
    return (means, centroids)
```

```python
import functools
import math

import jax
import jax.numpy as jnp
from jax import lax
from jax.experimental import pallas as pl
from jax.experimental.pallas import tpu as pltpu
from jax.sharding import PartitionSpec as P

CL_DEV = 1024
LANES = 128
F32 = jnp.float32
BF16 = jnp.bfloat16
I32 = jnp.int32


def full_body(points, assignment, sample_index):
    count_pts, features = points.shape
    size_gx = lax.axis_size("gx")
    rest = lax.axis_size("gy") * lax.axis_size("gz")
    devices = size_gx * rest
    capacity = 2 * count_pts // devices
    point_ids = jnp.arange(count_pts, dtype=jnp.int32)
    weight = jnp.zeros((count_pts,), jnp.float32).at[sample_index].add(1.0)
    owner = assignment // CL_DEV
    inside = assignment - owner * CL_DEV
    owner_hot = (owner[:, None] == jnp.arange(devices, dtype=jnp.int32)[None, :]).astype(
        jnp.float32
    )
    earlier = (point_ids[:, None] > point_ids[None, :]).astype(jnp.float32)
    before = jnp.dot(earlier, owner_hot, precision=lax.Precision.HIGHEST)
    place = jnp.sum(before * owner_hot, axis=1).astype(jnp.int32)
    slot = owner * capacity + place
    source = jnp.zeros((devices * capacity,), jnp.int32).at[slot].set(point_ids)
    filled = jnp.zeros((devices * capacity,), jnp.float32).at[slot].set(weight)
    tags = jnp.zeros((devices * capacity,), jnp.float32).at[slot].set(inside.astype(jnp.float32))
    rows = jnp.take(points, source, axis=0)
    got_rows, got_weight, got_tags = (
        lax.all_to_all(
            rows.reshape(devices, capacity, features),
            ("gx", "gy", "gz"),
            split_axis=0,
            concat_axis=0,
            tiled=True,
        ),
        lax.all_to_all(
            filled.reshape(devices, capacity),
            ("gx", "gy", "gz"),
            split_axis=0,
            concat_axis=0,
            tiled=True,
        ),
        lax.all_to_all(
            tags.reshape(devices, capacity),
            ("gx", "gy", "gz"),
            split_axis=0,
            concat_axis=0,
            tiled=True,
        ),
    )
    received = devices * capacity
    got_rows = got_rows.reshape(received, features)
    got_weight = got_weight.reshape(received)
    got_tags = got_tags.reshape(received)
    block_rows = math.gcd(received, 512)
    block_count = received // block_rows
    cluster_ids = jnp.arange(CL_DEV, dtype=jnp.float32)

    def accumulate(carry, index):
        totals, tally = carry
        start = index * block_rows
        rows_b = lax.dynamic_slice_in_dim(got_rows, start, block_rows, 0)
        weight_b = lax.dynamic_slice_in_dim(got_weight, start, block_rows, 0)
        tags_b = lax.dynamic_slice_in_dim(got_tags, start, block_rows, 0)
        onehot = (tags_b[:, None] == cluster_ids[None, :]).astype(jnp.float32) * weight_b[:, None]
        totals = totals + jnp.einsum("rk,rd->kd", onehot, rows_b, precision=lax.Precision.HIGHEST)
        tally = tally + jnp.sum(onehot, axis=0)
        return ((totals, tally), None)

    start_carry = (jnp.zeros((CL_DEV, features), jnp.float32), jnp.zeros((CL_DEV,), jnp.float32))
    (owned, owned_tally), unused = lax.scan(
        accumulate, start_carry, jnp.arange(block_count, dtype=jnp.int32)
    )
    means = owned / jnp.maximum(owned_tally, 1.0)[:, None]
    centroids = means / jnp.sqrt(jnp.sum(means * means, axis=1, keepdims=True) + 1e-06)
    return (means, centroids)


def shift_div(x, n):
    return lax.shift_right_logical(x, jnp.int32(n.bit_length() - 1))


def iota(shape, dim):
    return lax.broadcasted_iota(I32, shape, dim)


def as_bf16(mask):
    return jnp.where(mask, 1.0, 0.0).astype(BF16)


def nt_dot(a, b):
    return lax.dot_general(a, b, (((1,), (1,)), ((), ())), preferred_element_type=F32)


def nn_dot(a, b):
    return jnp.dot(a, b, preferred_element_type=F32)


def three(x):
    hi = x.astype(BF16)
    rest = x - hi.astype(F32)
    mid = rest.astype(BF16)
    low = (rest - mid.astype(F32)).astype(BF16)
    return hi, mid, low


def place(hot, group, chunks, room):
    groups = hot.shape[0]
    upper = as_bf16(iota((LANES, LANES), 0) < iota((LANES, LANES), 1))
    run = jnp.zeros((groups, 1), F32)
    places = []
    for c in range(chunks):
        h = hot[:, c * LANES : (c + 1) * LANES]
        before = nn_dot(h.astype(BF16), upper) + run
        places.append(jnp.sum(before * h, axis=0, keepdims=True))
        run = run + jnp.sum(h, axis=1, keepdims=True)
    return jnp.concatenate(places, axis=1), jnp.max(run)


def pack(x3, ids, weight, valid, group, groups, room, flag, chunks, write):
    lanes = chunks * LANES
    hot = jnp.where((iota((groups, lanes), 0) == group) & valid, 1.0, 0.0)
    pos, most = place(hot, group, chunks, room)
    over = jnp.where(most > room - 1, 1.0, 0.0)
    flag = jnp.maximum(flag, over)
    pos = pos.astype(I32)
    keep = valid & (pos < room - 1)
    slot = jnp.where(keep, group * room + pos, -1)
    pick = as_bf16(iota((groups * room, lanes), 0) == slot)
    out = nn_dot(pick, x3[0]) + nn_dot(pick, x3[1]) + nn_dot(pick, x3[2])
    tag_slot = jnp.where(keep, group * LANES + pos, -1)
    pick_tag = as_bf16(iota((groups * LANES, lanes), 0) == tag_slot)
    w = weight.astype(I32)
    parts = [
        shift_div(ids, 16384),
        shift_div(ids, 128) & 127,
        ids & 127,
        shift_div(w, 128),
        w & 127,
    ]
    row = iota((8, lanes), 0)
    stack = jnp.zeros((8, lanes), F32)
    for k, part in enumerate(parts):
        stack = jnp.where(row == k, part.astype(F32), stack)
    tags = nt_dot(stack.astype(BF16), pick_tag)
    tag_ids = tags[0:1] * 16384.0 + tags[1:2] * 128.0 + tags[2:3]
    tag_w = tags[3:4] * 128.0 + tags[4:5]
    flags = jnp.full((1, LANES), 1.0, F32) * flag
    for g in range(groups):
        write(
            g,
            out[g * room : (g + 1) * room],
            tag_ids[:, g * LANES : (g + 1) * LANES],
            tag_w[:, g * LANES : (g + 1) * LANES],
            flags,
        )
    return flag


def write_block(ref, at, room, rows, tag_ids, tag_w, flags):
    ref[at + (slice(0, room), slice(None))] = rows
    last = slice(room - 1, room)
    ref[at + (last, slice(0, LANES))] = tag_ids
    ref[at + (last, slice(LANES, 2 * LANES))] = tag_w
    ref[at + (last, slice(2 * LANES, 3 * LANES))] = flags


def split_owner(ids, sizes):
    n_gx, n_gy, n_gz = sizes
    owner = shift_div(ids, CL_DEV)
    gz = owner & (n_gz - 1)
    gy = shift_div(owner, n_gz) & (n_gy - 1)
    gx = shift_div(owner, n_gz * n_gy)
    return gy, gx * n_gz + gz


def prepare_kernel(sizes, rooms, my_ref, points_ref, assign_ref, index_ref, *outs):
    n_gx, n_gy, n_gz = sizes
    room_a, room_b = rooms
    a_refs, b_ref = outs[:n_gy], outs[n_gy]
    count_pts = points_ref.shape[0]
    half = points_ref.shape[1] // 2
    chunks = count_pts // LANES
    ids = assign_ref[...]
    hot = as_bf16(iota((count_pts, count_pts), 0) == index_ref[...])
    weight = nt_dot(jnp.ones((8, count_pts), BF16), hot)[0:1]
    weight_col = nn_dot(hot, jnp.ones((count_pts, LANES), BF16))
    valid = weight > 0.0
    wide = jnp.concatenate([weight_col] * (half // LANES), axis=1)
    gy, plane = split_owner(ids, sizes)
    shift = (gy - my_ref[0] + n_gy) & (n_gy - 1)
    pack(
        three(points_ref[:, :half] * wide), ids, weight, valid, shift, n_gy, room_a, jnp.float32(0.0),
        chunks, lambda g, *v: write_block(a_refs[g], (), room_a, *v),
    )
    pack(
        three(points_ref[:, half:] * wide), ids, weight, valid, plane, n_gx * n_gz, room_b,
        jnp.float32(0.0), chunks, lambda g, *v: write_block(b_ref, (g,), room_b, *v),
    )


def gathered(blocks):
    rows, ids, weight, flag = [], [], [], jnp.zeros((1, LANES), F32)
    for block in blocks:
        room, width = block.shape
        rows.append(block)
        if room < LANES:
            rows.append(jnp.zeros((LANES - room, width), F32))
        last = block[room - 1 : room]
        ids.append(last[:, :LANES])
        weight.append(last[:, LANES : 2 * LANES])
        flag = jnp.maximum(flag, last[:, 2 * LANES : 3 * LANES])
    return (
        jnp.concatenate(rows, axis=0),
        jnp.concatenate(ids, axis=1).astype(I32),
        jnp.concatenate(weight, axis=1),
        jnp.max(flag),
    )


def forward_kernel(sizes, rooms, my_ref, *refs):
    n_gx, n_gy, n_gz = sizes
    room_a, room_b = rooms
    n_plane = n_gx * n_gz
    a_in, b_in = refs[:n_gy], refs[n_gy]
    a_out, b_out = refs[n_gy + 1], refs[n_gy + 2 : 2 * n_gy + 2]
    rows_a, ids_a, weight_a, flag_a = gathered([r[...] for r in a_in])
    rows_b, ids_b, weight_b, flag_b = gathered([b_in[g] for g in range(n_plane)])
    flag = jnp.maximum(flag_a, flag_b)
    gy_b, unused = split_owner(ids_b, sizes)
    unused, plane_a = split_owner(ids_a, sizes)
    shift = (gy_b - my_ref[0] + n_gy) & (n_gy - 1)
    flag = pack(
        three(rows_b), ids_b, weight_b, weight_b > 0.0, shift, n_gy, room_b, flag, n_plane,
        lambda g, *v: write_block(b_out[g], (), room_b, *v),
    )
    pack(
        three(rows_a), ids_a, weight_a, weight_a > 0.0, plane_a, n_plane, room_a, flag, n_gy,
        lambda g, *v: write_block(a_out, (g,), room_a, *v),
    )


def finish_kernel(sizes, steps, my_ref, *refs):
    n_gx, n_gy, n_gz = sizes
    n_plane = n_gx * n_gz
    a_in, b_in = refs[0], refs[1 : n_gy + 1]
    means_ref, cent_ref = refs[n_gy + 1 : n_gy + 3]
    xa, xb, ta, tb = refs[n_gy + 3 :]
    block = means_ref.shape[0]
    half = means_ref.shape[1] // 2
    step = pl.program_id(0)

    @pl.when(step == 0)
    def _():
        base = my_ref[0] * CL_DEV
        for source, x, t in (
            ([a_in[g] for g in range(n_plane)], xa, ta),
            ([r[...] for r in b_in], xb, tb),
        ):
            rows, ids, weight, unused = gathered(source)
            for k, part in enumerate(three(rows)):
                x[k] = part
            w = weight.astype(I32)
            t[0:1, :] = jnp.where(w > 0, ids - base, -1)
            t[1:2, :] = w

    first = step * block
    totals = []
    for x, t in ((xa, ta), (xb, tb)):
        lanes = t.shape[1]
        hot = as_bf16(iota((block, lanes), 0) + first == t[0:1, :])
        totals.append(nn_dot(hot, x[0]) + nn_dot(hot, x[1]) + nn_dot(hot, x[2]))
    w = tb[1:2, :]
    lanes = tb.shape[1]
    high = jnp.broadcast_to(shift_div(w, 128).astype(F32), (LANES, lanes)).astype(BF16)
    low = jnp.broadcast_to((w & 127).astype(F32), (LANES, lanes)).astype(BF16)
    tally = nt_dot(hot, high) * 128.0 + nt_dot(hot, low)
    wide = jnp.concatenate([jnp.maximum(tally, 1.0)] * (half // LANES), axis=1)
    left, right = totals[0] / wide, totals[1] / wide
    square = jnp.sum(left * left + right * right, axis=1, keepdims=True)
    norm = jnp.sqrt(square + 1e-06)
    means_ref[:, :half] = left
    means_ref[:, half:] = right
    cent_ref[:, :half] = left / norm
    cent_ref[:, half:] = right / norm


VMEM_SPEC = pl.BlockSpec(memory_space=pltpu.VMEM)
SMEM_SPEC = pl.BlockSpec(memory_space=pltpu.SMEM)


def body(points, assignment, sample_index):
    count_pts, features = points.shape
    half = features // 2
    sizes = tuple(lax.axis_size(a) for a in ("gx", "gy", "gz"))
    n_gx, n_gy, n_gz = sizes
    n_plane = n_gx * n_gz
    devices = n_gx * n_gy * n_gz
    capacity = 2 * count_pts // devices

    def room(groups, slack, most):
        return min(8 * ((5 * count_pts // (8 * groups) + slack + 7) // 8), 8 * (most // 8 + 1), LANES)

    room_a1 = room(n_gy, count_pts // 16, n_plane * capacity)
    room_b1 = room(n_plane, count_pts // 16, n_gy * capacity)
    room_a2 = room(n_plane, count_pts * 5 // 64, n_gy * capacity)
    room_b2 = room(n_gy, count_pts * 3 // 32, n_plane * capacity)
    my_gx, my_gy, my_gz = (lax.axis_index(a) for a in ("gx", "gy", "gz"))
    gy_id = my_gy.astype(I32).reshape(1)
    me = ((my_gx * n_gy + my_gy) * n_gz + my_gz).astype(I32).reshape(1)

    def along_gy(blocks):
        return [blocks[0]] + [
            lax.ppermute(blocks[s], "gy", [(i, (i + s) % n_gy) for i in range(n_gy)])
            for s in range(1, n_gy)
        ]

    def in_plane(blocks):
        return lax.all_to_all(blocks, ("gx", "gz"), split_axis=0, concat_axis=0, tiled=True)

    def shape(*dims):
        return jax.ShapeDtypeStruct(dims, F32)

    sent = pl.pallas_call(
        functools.partial(prepare_kernel, sizes, (room_a1, room_b1)),
        in_specs=[SMEM_SPEC] + [VMEM_SPEC] * 3,
        out_specs=[VMEM_SPEC] * (n_gy + 1),
        out_shape=[shape(room_a1, half)] * n_gy + [shape(n_plane, room_b1, half)],
        name="prepare",
    )(gy_id, points, assignment.reshape(1, count_pts), sample_index.reshape(1, count_pts))
    a1 = along_gy(sent[:n_gy])
    b1 = in_plane(sent[n_gy])
    sent = pl.pallas_call(
        functools.partial(forward_kernel, sizes, (room_a2, room_b2)),
        in_specs=[SMEM_SPEC] + [VMEM_SPEC] * (n_gy + 1),
        out_specs=[VMEM_SPEC] * (n_gy + 1),
        out_shape=[shape(n_plane, room_a2, half)] + [shape(room_b2, half)] * n_gy,
        name="forward",
    )(gy_id, *a1, b1)
    b2 = along_gy(sent[1:])
    a2 = in_plane(sent[0])
    flag = jnp.max(a2[:, room_a2 - 1, 2 * LANES : 3 * LANES], axis=0)
    flags = along_gy([flag] * n_gy)
    over = functools.reduce(jnp.maximum, flags)[0] > 0.0

    def finish(points, assignment, sample_index, a2, *b2):
        steps = 4
        block = CL_DEV // steps
        lanes_a, lanes_b = n_plane * LANES, n_gy * LANES
        return tuple(
            pl.pallas_call(
                functools.partial(finish_kernel, sizes, steps),
                grid=(steps,),
                in_specs=[SMEM_SPEC] + [VMEM_SPEC] * (n_gy + 1),
                out_specs=[pl.BlockSpec((block, features), lambda i: (i, 0))] * 2,
                out_shape=[shape(CL_DEV, features)] * 2,
                scratch_shapes=[
                    pltpu.VMEM((3, lanes_a, half), BF16),
                    pltpu.VMEM((3, lanes_b, half), BF16),
                    pltpu.VMEM((8, lanes_a), I32),
                    pltpu.VMEM((8, lanes_b), I32),
                ],
                compiler_params=pltpu.CompilerParams(dimension_semantics=("arbitrary",)),
                name="finish",
            )(me, a2, *b2)
        )

    def again(points, assignment, sample_index, a2, *b2):
        return full_body(points, assignment, sample_index)

    return lax.cond(over, again, finish, points, assignment, sample_index, a2, *b2)


def solution(mesh):
    return jax.shard_map(
        body,
        mesh=mesh,
        in_specs=(P(("gx", "gy", "gz"), None), P(("gx", "gy", "gz")), P(("gx", "gy", "gz"))),
        out_specs=(P(("gx", "gy", "gz"), None), P(("gx", "gy", "gz"), None)),
        check_vma=False,
    )
```

```python
import functools
import math

import jax
import jax.numpy as jnp
from jax import lax
from jax.experimental import pallas as pl
from jax.experimental.pallas import tpu as pltpu
from jax.sharding import PartitionSpec as P


CL_DEV = 1024
LANES = 128
F32 = jnp.float32
BF16 = jnp.bfloat16
PARTS = 3
I32 = jnp.int32


def full_body(points, assignment, sample_index):
    count_pts, features = points.shape
    size_gx = lax.axis_size("gx")
    rest = lax.axis_size("gy") * lax.axis_size("gz")
    devices = size_gx * rest
    capacity = 2 * count_pts // devices
    point_ids = jnp.arange(count_pts, dtype=jnp.int32)
    weight = jnp.zeros((count_pts,), jnp.float32).at[sample_index].add(1.0)
    owner = assignment // CL_DEV
    inside = assignment - owner * CL_DEV
    owner_hot = (owner[:, None] == jnp.arange(devices, dtype=jnp.int32)[None, :]).astype(
        jnp.float32
    )
    earlier = (point_ids[:, None] > point_ids[None, :]).astype(jnp.float32)
    before = jnp.dot(earlier, owner_hot, precision=lax.Precision.HIGHEST)
    place = jnp.sum(before * owner_hot, axis=1).astype(jnp.int32)
    slot = owner * capacity + place
    source = jnp.zeros((devices * capacity,), jnp.int32).at[slot].set(point_ids)
    filled = jnp.zeros((devices * capacity,), jnp.float32).at[slot].set(weight)
    tags = jnp.zeros((devices * capacity,), jnp.float32).at[slot].set(inside.astype(jnp.float32))
    rows = jnp.take(points, source, axis=0)
    got_rows, got_weight, got_tags = (
        lax.all_to_all(
            rows.reshape(devices, capacity, features),
            ("gx", "gy", "gz"),
            split_axis=0,
            concat_axis=0,
            tiled=True,
        ),
        lax.all_to_all(
            filled.reshape(devices, capacity),
            ("gx", "gy", "gz"),
            split_axis=0,
            concat_axis=0,
            tiled=True,
        ),
        lax.all_to_all(
            tags.reshape(devices, capacity),
            ("gx", "gy", "gz"),
            split_axis=0,
            concat_axis=0,
            tiled=True,
        ),
    )
    received = devices * capacity
    got_rows = got_rows.reshape(received, features)
    got_weight = got_weight.reshape(received)
    got_tags = got_tags.reshape(received)
    block_rows = math.gcd(received, 512)
    block_count = received // block_rows
    cluster_ids = jnp.arange(CL_DEV, dtype=jnp.float32)

    def accumulate(carry, index):
        totals, tally = carry
        start = index * block_rows
        rows_b = lax.dynamic_slice_in_dim(got_rows, start, block_rows, 0)
        weight_b = lax.dynamic_slice_in_dim(got_weight, start, block_rows, 0)
        tags_b = lax.dynamic_slice_in_dim(got_tags, start, block_rows, 0)
        onehot = (tags_b[:, None] == cluster_ids[None, :]).astype(jnp.float32) * weight_b[:, None]
        totals = totals + jnp.einsum("rk,rd->kd", onehot, rows_b, precision=lax.Precision.HIGHEST)
        tally = tally + jnp.sum(onehot, axis=0)
        return ((totals, tally), None)

    start_carry = (jnp.zeros((CL_DEV, features), jnp.float32), jnp.zeros((CL_DEV,), jnp.float32))
    (owned, owned_tally), unused = lax.scan(
        accumulate, start_carry, jnp.arange(block_count, dtype=jnp.int32)
    )
    means = owned / jnp.maximum(owned_tally, 1.0)[:, None]
    centroids = means / jnp.sqrt(jnp.sum(means * means, axis=1, keepdims=True) + 1e-06)
    return (means, centroids)


def shift_div(x, n):
    return lax.shift_right_logical(x, jnp.int32(n.bit_length() - 1))


def iota(shape, dim):
    return lax.broadcasted_iota(I32, shape, dim)


def as_bf16(mask):
    return jnp.where(mask, 1.0, 0.0).astype(BF16)


def nt_dot(a, b):
    return lax.dot_general(a, b, (((1,), (1,)), ((), ())), preferred_element_type=F32)


def nn_dot(a, b):
    return jnp.dot(a, b, preferred_element_type=F32)


def split(x):
    parts = []
    for _ in range(PARTS):
        parts.append(x.astype(BF16))
        x = x - parts[-1].astype(F32)
    return parts


def place(hot):
    groups, lanes = hot.shape
    upper = as_bf16(iota((LANES, LANES), 0) < iota((LANES, LANES), 1))
    run = jnp.zeros((groups, 1), F32)
    places = []
    for start in range(0, lanes, LANES):
        width = min(LANES, lanes - start)
        h = hot[:, start : start + width]
        before = nn_dot(h.astype(BF16), upper[:width, :width]) + run
        places.append(jnp.sum(before * h, axis=0, keepdims=True))
        run = run + jnp.sum(h, axis=1, keepdims=True)
    return jnp.concatenate(places, axis=1), jnp.max(run)


def pack(parts, ids, weight, group, groups, room, write):
    lanes = ids.shape[1]
    valid = weight > 0.0
    hot = jnp.where((iota((groups, lanes), 0) == group) & valid, 1.0, 0.0)
    pos, most = place(hot)
    pos = pos.astype(I32)
    keep = valid & (pos < room - 1)
    slot = jnp.where(keep, group * room + pos, -1)
    pick = as_bf16(iota((groups * room, lanes), 0) == slot)
    out = functools.reduce(jnp.add, [nn_dot(pick, part) for part in parts])
    w = weight.astype(I32)
    pieces = [
        shift_div(ids, 16384),
        shift_div(ids, 128) & 127,
        ids & 127,
        shift_div(w, 128),
        w & 127,
    ]
    row = iota((8, lanes), 0)
    stack = jnp.zeros((8, lanes), F32)
    for k, piece in enumerate(pieces):
        stack = jnp.where(row == k, piece.astype(F32), stack)
    tags = nt_dot(stack.astype(BF16), pick)
    tag_ids = tags[0:1] * 16384.0 + tags[1:2] * 128.0 + tags[2:3]
    tag_w = tags[3:4] * 128.0 + tags[4:5]
    for g in range(groups):
        span = slice(g * room, (g + 1) * room)
        write(g, out[span], tag_ids[:, span], tag_w[:, span])
    return most


def flag_row(flag):
    return jnp.where(iota((1, LANES), 1) == LANES - 1, jnp.full((1, LANES), 1.0, F32) * flag, 0.0)


def padded(row):
    width = row.shape[1]
    if width == LANES:
        return row
    return jnp.concatenate([row, jnp.zeros((1, LANES - width), F32)], axis=1)


def write_block(ref, at, room, rows, tag_ids, tag_w):
    ref[at + (slice(0, room), slice(None))] = rows
    last = slice(room - 1, room)
    ref[at + (last, slice(0, LANES))] = padded(tag_ids)
    ref[at + (last, slice(LANES, 2 * LANES))] = padded(tag_w)


def write_news(ref, at, room, flag, counts):
    last = slice(room - 1, room)
    lane = iota((1, LANES), 1)
    ids = ref[at + (last, slice(0, LANES))]
    ref[at + (last, slice(0, LANES))] = jnp.where(lane == LANES - 1, flag_row(flag), ids)
    ref[at + (last, slice(2 * LANES, 3 * LANES))] = counts


def above(most, room):
    return jnp.where(most > room - 1, 1.0, 0.0)


def gy_shift(gy, me, sizes):
    _, n_gy, n_gz = sizes
    return (gy - (shift_div(me, n_gz) & (n_gy - 1)) + n_gy) & (n_gy - 1)


def split_owner(ids, sizes):
    _, n_gy, n_gz = sizes
    owner = shift_div(ids, CL_DEV)
    gz = owner & (n_gz - 1)
    gy = shift_div(owner, n_gz) & (n_gy - 1)
    gx = shift_div(owner, n_gz * n_gy)
    return gy, gx * n_gz + gz


def prepare_a_kernel(sizes, room, my_ref, x_ref, assign_ref, index_ref, *outs):
    _, n_gy, _ = sizes
    a_refs, weight_ref, wide_ref = outs[:n_gy], outs[n_gy], outs[n_gy + 1]
    count_pts, half = x_ref.shape
    ids = assign_ref[...]
    hot = as_bf16(iota((count_pts, count_pts), 0) == index_ref[...])
    weight = nt_dot(jnp.ones((8, count_pts), BF16), hot)[0:1]
    weight_ref[...] = weight
    weight_col = nn_dot(hot, jnp.ones((count_pts, LANES), BF16))
    wide_ref[...] = weight_col
    wide = jnp.concatenate([weight_col] * (half // LANES), axis=1)
    gy, _ = split_owner(ids, sizes)
    shift = gy_shift(gy, my_ref[0], sizes)
    most = pack(
        split(x_ref[...] * wide), ids, weight, shift, n_gy, room,
        lambda g, *v: write_block(a_refs[g], (), room, *v),
    )
    counts = demand(ids, weight)
    for g in range(n_gy):
        write_news(a_refs[g], (), room, above(most, room), counts)


def prepare_b_kernel(sizes, room, x_ref, assign_ref, weight_ref, wide_ref, b_ref):
    n_gx, _, n_gz = sizes
    half = x_ref.shape[1]
    ids, weight = assign_ref[...], weight_ref[...]
    wide = jnp.concatenate([wide_ref[...]] * (half // LANES), axis=1)
    _, plane = split_owner(ids, sizes)
    most = pack(
        split(x_ref[...] * wide), ids, weight, plane, n_gx * n_gz, room,
        lambda g, *v: write_block(b_ref, (g,), room, *v),
    )
    counts = demand(ids, weight)
    for g in range(n_gx * n_gz):
        write_news(b_ref, (g,), room, above(most, room), counts)


def demand(ids, weight):
    owner = shift_div(ids, CL_DEV)
    hot = as_bf16(iota((LANES, ids.shape[1]), 0) == owner)
    return nt_dot(jnp.where(jnp.broadcast_to(weight, (8, ids.shape[1])) > 0.0, 1.0, 0.0).astype(BF16), hot)[0:1]


def gathered(blocks):
    rows, ids, weight = [], [], []
    first, counts = jnp.zeros((1, LANES), F32), jnp.zeros((1, LANES), F32)
    for block in blocks:
        room = block.shape[0]
        rows.append(block)
        last = block[room - 1 : room]
        ids.append(last[:, :room])
        weight.append(last[:, LANES : LANES + room])
        first = jnp.maximum(first, last[:, :LANES])
        counts = counts + last[:, 2 * LANES : 3 * LANES]
    flag = jnp.max(jnp.where(iota((1, LANES), 1) == LANES - 1, first, 0.0))
    return (
        jnp.concatenate(rows, axis=0),
        jnp.concatenate(ids, axis=1).astype(I32),
        jnp.concatenate(weight, axis=1),
        flag,
        counts,
    )


def forward_b_kernel(sizes, room, my_ref, b_in, *b_out):
    n_gx, n_gy, n_gz = sizes
    rows, ids, weight, flag, counts = gathered([b_in[g] for g in range(n_gx * n_gz)])
    gy, _ = split_owner(ids, sizes)
    pack(
        split(rows), ids, weight, gy_shift(gy, my_ref[0], sizes), n_gy, room,
        lambda g, *v: write_block(b_out[g], (), room, *v),
    )
    flag = jnp.maximum(flag, above(jnp.max(counts), room))
    for g in range(n_gy):
        write_news(b_out[g], (), room, flag, counts)


def forward_a_kernel(sizes, room, *refs):
    n_gx, n_gy, n_gz = sizes
    a_in, a_out = refs[:n_gy], refs[n_gy]
    rows, ids, weight, flag, counts = gathered([r[...] for r in a_in])
    _, plane = split_owner(ids, sizes)
    pack(
        split(rows), ids, weight, plane, n_gx * n_gz, room,
        lambda g, *v: write_block(a_out, (g,), room, *v),
    )
    flag = jnp.maximum(flag, above(jnp.max(counts), room))
    for g in range(n_gx * n_gz):
        write_news(a_out, (g,), room, flag, counts)


def add_b_kernel(sizes, block, my_ref, *refs):
    _, n_gy, _ = sizes
    b_in, sum_ref, tally_ref, flag_ref = refs[:n_gy], refs[n_gy], refs[n_gy + 1], refs[n_gy + 2]
    rows, ids, weight, flag, _ = gathered([r[...] for r in b_in])
    flag_ref[...] = jnp.full((1, LANES), 1.0, F32) * flag
    parts = split(rows)
    w = weight.astype(I32)
    target = jnp.where(w > 0, ids - my_ref[0] * CL_DEV, -1)
    lanes = target.shape[1]
    high = jnp.broadcast_to(shift_div(w, 128).astype(F32), (LANES, lanes)).astype(BF16)
    low = jnp.broadcast_to((w & 127).astype(F32), (LANES, lanes)).astype(BF16)
    for first in range(0, CL_DEV, block):
        hot = as_bf16(iota((block, lanes), 0) + first == target)
        sum_ref[first : first + block] = functools.reduce(jnp.add, [nn_dot(hot, p) for p in parts])
        tally_ref[first : first + block] = nt_dot(hot, high) * 128.0 + nt_dot(hot, low)


def finish_kernel(
    sizes, my_ref, a_in, sum_ref, tally_ref, flag_b_ref, means_ref, cent_ref, flag_ref, x_ref, t_ref
):
    n_gx, _, n_gz = sizes
    block = means_ref.shape[0]
    half = means_ref.shape[1] // 2
    step = pl.program_id(0)

    @pl.when(step == 0)
    def _():
        rows, ids, weight, flag, _ = gathered([a_in[g] for g in range(n_gx * n_gz)])
        flag_ref[0, 0] = jnp.maximum(flag, jnp.max(flag_b_ref[...]))
        for k, part in enumerate(split(rows)):
            x_ref[k] = part
        t_ref[0:1, :] = jnp.where(weight > 0.0, ids - my_ref[0] * CL_DEV, -1)

    first = pl.multiple_of(step * block, block)
    lanes = t_ref.shape[1]
    hot = as_bf16(iota((block, lanes), 0) + first == t_ref[0:1, :])
    left = functools.reduce(jnp.add, [nn_dot(hot, x_ref[k]) for k in range(PARTS)])
    right = sum_ref[pl.ds(first, block)]
    share = 1.0 / jnp.maximum(tally_ref[pl.ds(first, block)], 1.0)
    wide = jnp.concatenate([share] * (half // LANES), axis=1)
    left, right = left * wide, right * wide
    square = jnp.sum(left * left + right * right, axis=1, keepdims=True)
    scale = 1.0 / jnp.sqrt(square + 1e-06)
    means_ref[:, :half] = left
    means_ref[:, half:] = right
    cent_ref[:, :half] = left * scale
    cent_ref[:, half:] = right * scale


VMEM_SPEC = pl.BlockSpec(memory_space=pltpu.VMEM)
SMEM_SPEC = pl.BlockSpec(memory_space=pltpu.SMEM)


def body(points, assignment, sample_index):
    count_pts, features = points.shape
    half = features // 2
    sizes = tuple(lax.axis_size(a) for a in ("gx", "gy", "gz"))
    n_gx, n_gy, n_gz = sizes
    n_plane = n_gx * n_gz
    devices = n_gx * n_gy * n_gz
    capacity = 2 * count_pts // devices

    def room(groups, slack, most):
        return min(8 * ((5 * count_pts // (8 * groups) + slack + 7) // 8), 8 * (most // 8 + 1), LANES)

    room_a1 = room(n_gy, count_pts // 16, n_plane * capacity)
    room_b1 = room(n_plane, count_pts // 16, n_gy * capacity)
    room_a2 = room(n_plane, count_pts * 5 // 64, n_gy * capacity)
    room_b2 = room(n_gy, count_pts * 3 // 32, n_plane * capacity)
    my_gx, my_gy, my_gz = (lax.axis_index(a) for a in ("gx", "gy", "gz"))
    me = ((my_gx * n_gy + my_gy) * n_gz + my_gz).astype(I32).reshape(1)

    def along_gy(blocks):
        out = [blocks[0]]
        for s in range(1, n_gy):
            out.append(lax.ppermute(blocks[s], "gy", [(i, (i + s) % n_gy) for i in range(n_gy)]))
        return out

    def in_plane(blocks):
        return lax.all_to_all(blocks, ("gx", "gz"), split_axis=0, concat_axis=0, tiled=True)

    def cost(us):
        return pl.CostEstimate(flops=us * 7_000_000, bytes_accessed=1 << 20, transcendentals=0)

    def vmem(mib, **others):
        return pltpu.CompilerParams(vmem_limit_bytes=mib << 20, **others)

    def shape(*dims):
        return jax.ShapeDtypeStruct(dims, F32)

    assign = assignment.reshape(1, count_pts)
    sent = pl.pallas_call(
        functools.partial(prepare_a_kernel, sizes, room_a1),
        grid=(1,),
        in_specs=[SMEM_SPEC, pl.BlockSpec((count_pts, half), lambda i: (0, 0))] + [VMEM_SPEC] * 2,
        out_specs=[VMEM_SPEC] * (n_gy + 2),
        out_shape=[shape(room_a1, half)] * n_gy + [shape(1, count_pts), shape(count_pts, LANES)],
        compiler_params=vmem(12),
        cost_estimate=cost(3),
        name="prepare_a",
    )(me, points, assign, sample_index.reshape(1, count_pts))
    a1 = along_gy(sent[:n_gy])
    sent_b = pl.pallas_call(
        functools.partial(prepare_b_kernel, sizes, room_b1),
        grid=(1,),
        in_specs=[pl.BlockSpec((count_pts, half), lambda i: (0, 1))] + [VMEM_SPEC] * 3,
        out_specs=VMEM_SPEC,
        out_shape=shape(n_plane, room_b1, half),
        compiler_params=vmem(12),
        cost_estimate=cost(3),
        name="prepare_b",
    )(points, assign, sent[n_gy], sent[n_gy + 1])
    b1 = in_plane(sent_b)
    sent_a = pl.pallas_call(
        functools.partial(forward_a_kernel, sizes, room_a2),
        in_specs=[VMEM_SPEC] * n_gy,
        out_specs=VMEM_SPEC,
        out_shape=shape(n_plane, room_a2, half),
        compiler_params=vmem(8),
        cost_estimate=cost(3),
        name="forward_a",
    )(*a1)
    a2 = in_plane(sent_a)
    sent_b = pl.pallas_call(
        functools.partial(forward_b_kernel, sizes, room_b2),
        in_specs=[SMEM_SPEC, VMEM_SPEC],
        out_specs=[VMEM_SPEC] * n_gy,
        out_shape=[shape(room_b2, half)] * n_gy,
        compiler_params=vmem(8),
        cost_estimate=cost(3),
        name="forward_b",
    )(me, b1)
    b2 = along_gy(sent_b)
    block = CL_DEV // 4
    sum_b, tally, flag_b = pl.pallas_call(
        functools.partial(add_b_kernel, sizes, block),
        in_specs=[SMEM_SPEC] + [VMEM_SPEC] * n_gy,
        out_specs=[VMEM_SPEC] * 3,
        out_shape=[shape(CL_DEV, half), shape(CL_DEV, LANES), shape(1, LANES)],
        compiler_params=vmem(8),
        cost_estimate=cost(3),
        name="add_b",
    )(me, *b2)
    steps = 4
    block = CL_DEV // steps
    lanes_a = n_plane * room_a2
    means, centroids, over = pl.pallas_call(
        functools.partial(finish_kernel, sizes),
        grid=(steps,),
        in_specs=[SMEM_SPEC] + [VMEM_SPEC] * 4,
        out_specs=[pl.BlockSpec((block, features), lambda i: (i, 0))] * 2 + [SMEM_SPEC],
        out_shape=[shape(CL_DEV, features)] * 2 + [shape(1, 1)],
        scratch_shapes=[pltpu.VMEM((PARTS, lanes_a, half), BF16), pltpu.VMEM((8, lanes_a), I32)],
        compiler_params=vmem(16, dimension_semantics=("arbitrary",)),
        cost_estimate=cost(6),
        name="finish",
    )(me, a2, sum_b, tally, flag_b)

    def again(carry):
        return (jnp.float32(0.0),) + full_body(points, assignment, sample_index)

    return lax.while_loop(lambda carry: carry[0] > 0.0, again, (over[0, 0], means, centroids))[1:]


def solution(mesh):
    return jax.shard_map(
        body,
        mesh=mesh,
        in_specs=(P(("gx", "gy", "gz"), None), P(("gx", "gy", "gz")), P(("gx", "gy", "gz"))),
        out_specs=(P(("gx", "gy", "gz"), None), P(("gx", "gy", "gz"), None)),
        check_vma=False,
    )
```

```python
import functools
import math

import jax
import jax.numpy as jnp
from jax import lax
from jax.experimental import pallas as pl
from jax.experimental.pallas import tpu as pltpu
from jax.sharding import PartitionSpec as P


CL_DEV = 1024
LANES = 128
F32 = jnp.float32
BF16 = jnp.bfloat16
PARTS = 2
I32 = jnp.int32


def full_body(points, assignment, sample_index):
    count_pts, features = points.shape
    size_gx = lax.axis_size("gx")
    rest = lax.axis_size("gy") * lax.axis_size("gz")
    devices = size_gx * rest
    capacity = 2 * count_pts // devices
    point_ids = jnp.arange(count_pts, dtype=jnp.int32)
    weight = jnp.zeros((count_pts,), jnp.float32).at[sample_index].add(1.0)
    owner = assignment // CL_DEV
    inside = assignment - owner * CL_DEV
    owner_hot = (owner[:, None] == jnp.arange(devices, dtype=jnp.int32)[None, :]).astype(
        jnp.float32
    )
    earlier = (point_ids[:, None] > point_ids[None, :]).astype(jnp.float32)
    before = jnp.dot(earlier, owner_hot, precision=lax.Precision.HIGHEST)
    place = jnp.sum(before * owner_hot, axis=1).astype(jnp.int32)
    slot = owner * capacity + place
    source = jnp.zeros((devices * capacity,), jnp.int32).at[slot].set(point_ids)
    filled = jnp.zeros((devices * capacity,), jnp.float32).at[slot].set(weight)
    tags = jnp.zeros((devices * capacity,), jnp.float32).at[slot].set(inside.astype(jnp.float32))
    rows = jnp.take(points, source, axis=0)
    got_rows, got_weight, got_tags = (
        lax.all_to_all(
            rows.reshape(devices, capacity, features),
            ("gx", "gy", "gz"),
            split_axis=0,
            concat_axis=0,
            tiled=True,
        ),
        lax.all_to_all(
            filled.reshape(devices, capacity),
            ("gx", "gy", "gz"),
            split_axis=0,
            concat_axis=0,
            tiled=True,
        ),
        lax.all_to_all(
            tags.reshape(devices, capacity),
            ("gx", "gy", "gz"),
            split_axis=0,
            concat_axis=0,
            tiled=True,
        ),
    )
    received = devices * capacity
    got_rows = got_rows.reshape(received, features)
    got_weight = got_weight.reshape(received)
    got_tags = got_tags.reshape(received)
    block_rows = math.gcd(received, 512)
    block_count = received // block_rows
    cluster_ids = jnp.arange(CL_DEV, dtype=jnp.float32)

    def accumulate(carry, index):
        totals, tally = carry
        start = index * block_rows
        rows_b = lax.dynamic_slice_in_dim(got_rows, start, block_rows, 0)
        weight_b = lax.dynamic_slice_in_dim(got_weight, start, block_rows, 0)
        tags_b = lax.dynamic_slice_in_dim(got_tags, start, block_rows, 0)
        onehot = (tags_b[:, None] == cluster_ids[None, :]).astype(jnp.float32) * weight_b[:, None]
        totals = totals + jnp.einsum("rk,rd->kd", onehot, rows_b, precision=lax.Precision.HIGHEST)
        tally = tally + jnp.sum(onehot, axis=0)
        return ((totals, tally), None)

    start_carry = (jnp.zeros((CL_DEV, features), jnp.float32), jnp.zeros((CL_DEV,), jnp.float32))
    (owned, owned_tally), unused = lax.scan(
        accumulate, start_carry, jnp.arange(block_count, dtype=jnp.int32)
    )
    means = owned / jnp.maximum(owned_tally, 1.0)[:, None]
    centroids = means / jnp.sqrt(jnp.sum(means * means, axis=1, keepdims=True) + 1e-06)
    return (means, centroids)


def shift_div(x, n):
    return lax.shift_right_logical(x, jnp.int32(n.bit_length() - 1))


def iota(shape, dim):
    return lax.broadcasted_iota(I32, shape, dim)


def as_bf16(mask):
    return jnp.where(mask, 1.0, 0.0).astype(BF16)


def nt_dot(a, b):
    return lax.dot_general(a, b, (((1,), (1,)), ((), ())), preferred_element_type=F32)


def nn_dot(a, b):
    return jnp.dot(a, b, preferred_element_type=F32)


def split(x):
    parts = []
    for _ in range(PARTS):
        parts.append(x.astype(BF16))
        x = x - parts[-1].astype(F32)
    return jnp.concatenate(parts, axis=1)


def chosen(hot, parts):
    both = nn_dot(hot, parts)
    width = both.shape[1] // PARTS
    return functools.reduce(jnp.add, [both[:, k * width : (k + 1) * width] for k in range(PARTS)])


def place(hot):
    groups, lanes = hot.shape
    upper = as_bf16(iota((LANES, LANES), 0) < iota((LANES, LANES), 1))
    run = jnp.zeros((groups, 1), F32)
    places = []
    for start in range(0, lanes, LANES):
        width = min(LANES, lanes - start)
        h = hot[:, start : start + width]
        before = nn_dot(h.astype(BF16), upper[:width, :width]) + run
        places.append(jnp.sum(before * h, axis=0, keepdims=True))
        run = run + jnp.sum(h, axis=1, keepdims=True)
    return jnp.concatenate(places, axis=1), jnp.max(run)


def pack(parts, ids, weight, group, groups, room, write):
    lanes = ids.shape[1]
    valid = weight > 0.0
    hot = jnp.where((iota((groups, lanes), 0) == group) & valid, 1.0, 0.0)
    pos, most = place(hot)
    pos = pos.astype(I32)
    keep = valid & (pos < room - 1)
    slot = jnp.where(keep, group * room + pos, -1)
    pick = as_bf16(iota((groups * room, lanes), 0) == slot)
    out = chosen(pick, parts)
    w = weight.astype(I32)
    pieces = [
        shift_div(ids, 16384),
        shift_div(ids, 128) & 127,
        ids & 127,
        shift_div(w, 128),
        w & 127,
    ]
    row = iota((8, lanes), 0)
    stack = jnp.zeros((8, lanes), F32)
    for k, piece in enumerate(pieces):
        stack = jnp.where(row == k, piece.astype(F32), stack)
    tags = nt_dot(stack.astype(BF16), pick)
    tag_ids = tags[0:1] * 16384.0 + tags[1:2] * 128.0 + tags[2:3]
    tag_w = tags[3:4] * 128.0 + tags[4:5]
    for g in range(groups):
        span = slice(g * room, (g + 1) * room)
        write(g, out[span], tag_ids[:, span], tag_w[:, span])
    return most


def flag_row(flag):
    return jnp.where(iota((1, LANES), 1) == LANES - 1, jnp.full((1, LANES), 1.0, F32) * flag, 0.0)


def padded(row):
    width = row.shape[1]
    if width == LANES:
        return row
    return jnp.concatenate([row, jnp.zeros((1, LANES - width), F32)], axis=1)


def write_block(ref, at, room, rows, tag_ids, tag_w):
    ref[at + (slice(0, room), slice(None))] = rows
    last = slice(room - 1, room)
    ref[at + (last, slice(0, LANES))] = padded(tag_ids)
    ref[at + (last, slice(LANES, 2 * LANES))] = padded(tag_w)


def write_news(ref, at, room, flag, counts):
    last = slice(room - 1, room)
    lane = iota((1, LANES), 1)
    ids = ref[at + (last, slice(0, LANES))]
    ref[at + (last, slice(0, LANES))] = jnp.where(lane == LANES - 1, flag_row(flag), ids)
    ref[at + (last, slice(2 * LANES, 3 * LANES))] = counts


def above(most, room):
    return jnp.where(most > room - 1, 1.0, 0.0)


def split_device(device, sizes):
    _, n_gy, n_gz = sizes
    gz = device & (n_gz - 1)
    gy = shift_div(device, n_gz) & (n_gy - 1)
    gx = shift_div(device, n_gz * n_gy)
    return gy, gx * n_gz + gz


def offsets(ids, me, sizes):
    gy, plane = split_device(shift_div(ids, CL_DEV), sizes)
    my_gy, my_plane = split_device(me, sizes)
    return gy ^ my_gy, plane ^ my_plane


def prepare_a_kernel(sizes, room, my_ref, x_ref, assign_ref, index_ref, *outs):
    _, n_gy, _ = sizes
    a_refs, weight_ref, wide_ref = outs[:n_gy], outs[n_gy], outs[n_gy + 1]
    count_pts, half = x_ref.shape
    ids = assign_ref[...]
    hot = as_bf16(iota((count_pts, count_pts), 0) == index_ref[...])
    weight = nt_dot(jnp.ones((8, count_pts), BF16), hot)[0:1]
    weight_ref[...] = weight
    weight_col = nn_dot(hot, jnp.ones((count_pts, LANES), BF16))
    wide_ref[...] = weight_col
    wide = jnp.concatenate([weight_col] * (half // LANES), axis=1)
    along, _ = offsets(ids, my_ref[0], sizes)
    most = pack(
        split(x_ref[...] * wide), ids, weight, along, n_gy, room,
        lambda g, *v: write_block(a_refs[g], (), room, *v),
    )
    counts = demand(ids, weight)
    for g in range(n_gy):
        write_news(a_refs[g], (), room, above(most, room), counts)


def prepare_b_kernel(sizes, room, my_ref, x_ref, assign_ref, weight_ref, wide_ref, *b_refs):
    half = x_ref.shape[1]
    ids, weight = assign_ref[...], weight_ref[...]
    wide = jnp.concatenate([wide_ref[...]] * (half // LANES), axis=1)
    _, across = offsets(ids, my_ref[0], sizes)
    most = pack(
        split(x_ref[...] * wide), ids, weight, across, len(b_refs), room,
        lambda g, *v: write_block(b_refs[g], (), room, *v),
    )
    counts = demand(ids, weight)
    for ref in b_refs:
        write_news(ref, (), room, above(most, room), counts)


def demand(ids, weight):
    owner = shift_div(ids, CL_DEV)
    hot = as_bf16(iota((LANES, ids.shape[1]), 0) == owner)
    return nt_dot(jnp.where(jnp.broadcast_to(weight, (8, ids.shape[1])) > 0.0, 1.0, 0.0).astype(BF16), hot)[0:1]


def gathered(blocks):
    rows, ids, weight = [], [], []
    first, counts = jnp.zeros((1, LANES), F32), jnp.zeros((1, LANES), F32)
    for block in blocks:
        room = block.shape[0]
        rows.append(block)
        last = block[room - 1 : room]
        ids.append(last[:, :room])
        weight.append(last[:, LANES : LANES + room])
        first = jnp.maximum(first, last[:, :LANES])
        counts = counts + last[:, 2 * LANES : 3 * LANES]
    flag = jnp.max(jnp.where(iota((1, LANES), 1) == LANES - 1, first, 0.0))
    return (
        jnp.concatenate(rows, axis=0),
        jnp.concatenate(ids, axis=1).astype(I32),
        jnp.concatenate(weight, axis=1),
        flag,
        counts,
    )


def forward_kernel(sizes, room, to_plane, count_in, my_ref, *refs):
    outs = refs[count_in:]
    rows, ids, weight, flag, counts = gathered([r[...] for r in refs[:count_in]])
    along, across = offsets(ids, my_ref[0], sizes)
    pack(
        split(rows), ids, weight, across if to_plane else along, len(outs), room,
        lambda g, *v: write_block(outs[g], (), room, *v),
    )
    flag = jnp.maximum(flag, above(jnp.max(counts), room))
    for ref in outs:
        write_news(ref, (), room, flag, counts)


def add_kernel(block, my_ref, *refs):
    blocks, (sum_ref, tally_ref, flag_ref) = refs[:-3], refs[-3:]
    rows, ids, weight, flag, _ = gathered([r[...] for r in blocks])
    flag_ref[...] = jnp.full((1, LANES), 1.0, F32) * flag
    parts = split(rows)
    w = weight.astype(I32)
    target = jnp.where(w > 0, ids - my_ref[0] * CL_DEV, -1)
    lanes = target.shape[1]
    high = jnp.broadcast_to(shift_div(w, 128).astype(F32), (LANES, lanes)).astype(BF16)
    low = jnp.broadcast_to((w & 127).astype(F32), (LANES, lanes)).astype(BF16)
    for first in range(0, CL_DEV, block):
        hot = as_bf16(iota((block, lanes), 0) + first == target)
        sum_ref[first : first + block] = chosen(hot, parts)
        tally = nt_dot(hot, high) * 128.0 + nt_dot(hot, low)
        tally_ref[first : first + block] = 1.0 / jnp.maximum(tally, 1.0)


def finish_kernel(count_in, my_ref, *refs):
    blocks = refs[:count_in]
    sum_ref, share_ref, flag_a_ref, means_ref, cent_ref, flag_ref, x_ref, t_ref = refs[count_in:]
    block = means_ref.shape[0]
    half = means_ref.shape[1] // 2
    step = pl.program_id(0)

    @pl.when(step == 0)
    def _():
        rows, ids, weight, flag, _ = gathered([r[...] for r in blocks])
        flag_ref[0, 0] = jnp.maximum(flag, jnp.max(flag_a_ref[...]))
        x_ref[...] = split(rows)
        t_ref[0:1, :] = jnp.where(weight > 0.0, ids - my_ref[0] * CL_DEV, -1)

    first = pl.multiple_of(step * block, block)
    lanes = t_ref.shape[1]
    hot = as_bf16(iota((block, lanes), 0) + first == t_ref[0:1, :])
    right = chosen(hot, x_ref[...])
    left = sum_ref[pl.ds(first, block)]
    wide = jnp.concatenate([share_ref[pl.ds(first, block)]] * (half // LANES), axis=1)
    left, right = left * wide, right * wide
    square = jnp.sum(left * left + right * right, axis=1, keepdims=True)
    scale = 1.0 / jnp.sqrt(square + 1e-06)
    means_ref[:, :half] = left
    means_ref[:, half:] = right
    cent_ref[:, :half] = left * scale
    cent_ref[:, half:] = right * scale


VMEM_SPEC = pl.BlockSpec(memory_space=pltpu.VMEM)
SMEM_SPEC = pl.BlockSpec(memory_space=pltpu.SMEM)


def body(points, assignment, sample_index):
    count_pts, features = points.shape
    half = features // 2
    sizes = tuple(lax.axis_size(a) for a in ("gx", "gy", "gz"))
    n_gx, n_gy, n_gz = sizes
    n_plane = n_gx * n_gz
    devices = n_gx * n_gy * n_gz
    capacity = 2 * count_pts // devices

    def room(groups, slack, most):
        return min(8 * ((5 * count_pts // (8 * groups) + slack + 7) // 8), 8 * (most // 8 + 1), LANES)

    room_a1 = room(n_gy, count_pts // 16, n_plane * capacity)
    room_b1 = room(n_plane, count_pts // 16, n_gy * capacity)
    room_a2 = room(n_plane, count_pts * 5 // 64, n_gy * capacity)
    room_b2 = room(n_gy, count_pts * 3 // 32, n_plane * capacity)
    my_gx, my_gy, my_gz = (lax.axis_index(a) for a in ("gx", "gy", "gz"))
    me = ((my_gx * n_gy + my_gy) * n_gz + my_gz).astype(I32).reshape(1)

    def exchange(blocks, axes):
        out = [blocks[0]]
        for r in range(1, len(blocks)):
            out.append(lax.ppermute(blocks[r], axes, [(i, i ^ r) for i in range(len(blocks))]))
        return out

    def cost(us):
        return pl.CostEstimate(flops=us * 7_000_000, bytes_accessed=1 << 20, transcendentals=0)

    def vmem(mib, **others):
        return pltpu.CompilerParams(vmem_limit_bytes=mib << 20, **others)

    def shape(*dims):
        return jax.ShapeDtypeStruct(dims, F32)

    assign = assignment.reshape(1, count_pts)
    assign = assignment.reshape(1, count_pts)
    sent = pl.pallas_call(
        functools.partial(prepare_a_kernel, sizes, room_a1),
        grid=(1,),
        in_specs=[SMEM_SPEC, pl.BlockSpec((count_pts, half), lambda i: (0, 0))] + [VMEM_SPEC] * 2,
        out_specs=[VMEM_SPEC] * (n_gy + 2),
        out_shape=[shape(room_a1, half)] * n_gy + [shape(1, count_pts), shape(count_pts, LANES)],
        compiler_params=vmem(12),
        cost_estimate=cost(3),
        name="prepare_a",
    )(me, points, assign, sample_index.reshape(1, count_pts))
    a1 = exchange(sent[:n_gy], "gy")
    sent_b = pl.pallas_call(
        functools.partial(prepare_b_kernel, sizes, room_b1),
        grid=(1,),
        in_specs=[SMEM_SPEC, pl.BlockSpec((count_pts, half), lambda i: (0, 1))] + [VMEM_SPEC] * 3,
        out_specs=[VMEM_SPEC] * n_plane,
        out_shape=[shape(room_b1, half)] * n_plane,
        compiler_params=vmem(12),
        cost_estimate=cost(3),
        name="prepare_b",
    )(me, points, assign, sent[n_gy], sent[n_gy + 1])
    b1 = exchange(sent_b, ("gx", "gz"))

    def forward(blocks, to_plane, room):
        count = n_plane if to_plane else n_gy
        return pl.pallas_call(
            functools.partial(forward_kernel, sizes, room, to_plane, len(blocks)),
            in_specs=[SMEM_SPEC] + [VMEM_SPEC] * len(blocks),
            out_specs=[VMEM_SPEC] * count,
            out_shape=[shape(room, half)] * count,
            compiler_params=vmem(8),
            cost_estimate=cost(3),
        )(me, *blocks)

    a2 = exchange(forward(a1, True, room_a2), ("gx", "gz"))
    b2 = exchange(forward(b1, False, room_b2), "gy")
    sum_a, share, flag_a = pl.pallas_call(
        functools.partial(add_kernel, CL_DEV // 4),
        in_specs=[SMEM_SPEC] + [VMEM_SPEC] * n_plane,
        out_specs=[VMEM_SPEC] * 3,
        out_shape=[shape(CL_DEV, half), shape(CL_DEV, LANES), shape(1, LANES)],
        compiler_params=vmem(10),
        cost_estimate=cost(3),
        name="add_a",
    )(me, *a2)
    steps = 4
    block = CL_DEV // steps
    lanes_b = n_gy * room_b2
    means, centroids, over = pl.pallas_call(
        functools.partial(finish_kernel, n_gy),
        grid=(steps,),
        in_specs=[SMEM_SPEC] + [VMEM_SPEC] * (n_gy + 3),
        out_specs=[pl.BlockSpec((block, features), lambda i: (i, 0))] * 2 + [SMEM_SPEC],
        out_shape=[shape(CL_DEV, features)] * 2 + [shape(1, 1)],
        scratch_shapes=[pltpu.VMEM((lanes_b, PARTS * half), BF16), pltpu.VMEM((8, lanes_b), I32)],
        compiler_params=vmem(16, dimension_semantics=("arbitrary",)),
        cost_estimate=cost(6),
        name="finish",
    )(me, *b2, sum_a, share, flag_a)

    def again(carry):
        return (jnp.float32(0.0),) + full_body(points, assignment, sample_index)

    return lax.while_loop(lambda carry: carry[0] > 0.0, again, (over[0, 0], means, centroids))[1:]


def solution(mesh):
    return jax.shard_map(
        body,
        mesh=mesh,
        in_specs=(P(("gx", "gy", "gz"), None), P(("gx", "gy", "gz")), P(("gx", "gy", "gz"))),
        out_specs=(P(("gx", "gy", "gz"), None), P(("gx", "gy", "gz"), None)),
        check_vma=False,
    )
```

```python
import functools
import math

import jax
import jax.numpy as jnp
from jax import lax
from jax.experimental import pallas as pl
from jax.experimental.pallas import tpu as pltpu
from jax.sharding import PartitionSpec as P


CL_DEV = 1024
LANES = 128
F32 = jnp.float32
BF16 = jnp.bfloat16
PARTS = 2
I32 = jnp.int32


def full_body(points, assignment, sample_index):
    count_pts, features = points.shape
    size_gx = lax.axis_size("gx")
    rest = lax.axis_size("gy") * lax.axis_size("gz")
    devices = size_gx * rest
    capacity = 2 * count_pts // devices
    point_ids = jnp.arange(count_pts, dtype=jnp.int32)
    weight = jnp.zeros((count_pts,), jnp.float32).at[sample_index].add(1.0)
    owner = assignment // CL_DEV
    inside = assignment - owner * CL_DEV
    owner_hot = (owner[:, None] == jnp.arange(devices, dtype=jnp.int32)[None, :]).astype(
        jnp.float32
    )
    earlier = (point_ids[:, None] > point_ids[None, :]).astype(jnp.float32)
    before = jnp.dot(earlier, owner_hot, precision=lax.Precision.HIGHEST)
    place = jnp.sum(before * owner_hot, axis=1).astype(jnp.int32)
    slot = owner * capacity + place
    source = jnp.zeros((devices * capacity,), jnp.int32).at[slot].set(point_ids)
    filled = jnp.zeros((devices * capacity,), jnp.float32).at[slot].set(weight)
    tags = jnp.zeros((devices * capacity,), jnp.float32).at[slot].set(inside.astype(jnp.float32))
    rows = jnp.take(points, source, axis=0)
    got_rows, got_weight, got_tags = (
        lax.all_to_all(
            rows.reshape(devices, capacity, features),
            ("gx", "gy", "gz"),
            split_axis=0,
            concat_axis=0,
            tiled=True,
        ),
        lax.all_to_all(
            filled.reshape(devices, capacity),
            ("gx", "gy", "gz"),
            split_axis=0,
            concat_axis=0,
            tiled=True,
        ),
        lax.all_to_all(
            tags.reshape(devices, capacity),
            ("gx", "gy", "gz"),
            split_axis=0,
            concat_axis=0,
            tiled=True,
        ),
    )
    received = devices * capacity
    got_rows = got_rows.reshape(received, features)
    got_weight = got_weight.reshape(received)
    got_tags = got_tags.reshape(received)
    block_rows = math.gcd(received, 512)
    block_count = received // block_rows
    cluster_ids = jnp.arange(CL_DEV, dtype=jnp.float32)

    def accumulate(carry, index):
        totals, tally = carry
        start = index * block_rows
        rows_b = lax.dynamic_slice_in_dim(got_rows, start, block_rows, 0)
        weight_b = lax.dynamic_slice_in_dim(got_weight, start, block_rows, 0)
        tags_b = lax.dynamic_slice_in_dim(got_tags, start, block_rows, 0)
        onehot = (tags_b[:, None] == cluster_ids[None, :]).astype(jnp.float32) * weight_b[:, None]
        totals = totals + jnp.einsum("rk,rd->kd", onehot, rows_b, precision=lax.Precision.HIGHEST)
        tally = tally + jnp.sum(onehot, axis=0)
        return ((totals, tally), None)

    start_carry = (jnp.zeros((CL_DEV, features), jnp.float32), jnp.zeros((CL_DEV,), jnp.float32))
    (owned, owned_tally), unused = lax.scan(
        accumulate, start_carry, jnp.arange(block_count, dtype=jnp.int32)
    )
    means = owned / jnp.maximum(owned_tally, 1.0)[:, None]
    centroids = means / jnp.sqrt(jnp.sum(means * means, axis=1, keepdims=True) + 1e-06)
    return (means, centroids)


def shift_div(x, n):
    return lax.shift_right_logical(x, jnp.int32(n.bit_length() - 1))


def iota(shape, dim):
    return lax.broadcasted_iota(I32, shape, dim)


def as_bf16(mask):
    return jnp.where(mask, 1.0, 0.0).astype(BF16)


def nt_dot(a, b):
    return lax.dot_general(a, b, (((1,), (1,)), ((), ())), preferred_element_type=F32)


def nn_dot(a, b):
    return jnp.dot(a, b, preferred_element_type=F32)


def split(x):
    parts = []
    for _ in range(PARTS):
        parts.append(x.astype(BF16))
        x = x - parts[-1].astype(F32)
    return jnp.concatenate(parts, axis=1)


def chosen(hot, parts):
    both = nn_dot(hot, parts)
    width = both.shape[1] // PARTS
    return functools.reduce(jnp.add, [both[:, k * width : (k + 1) * width] for k in range(PARTS)])


def place(hot):
    groups, lanes = hot.shape
    upper = as_bf16(iota((LANES, LANES), 0) < iota((LANES, LANES), 1))
    run = jnp.zeros((groups, 1), F32)
    places = []
    for start in range(0, lanes, LANES):
        width = min(LANES, lanes - start)
        h = hot[:, start : start + width]
        before = nn_dot(h.astype(BF16), upper[:width, :width]) + run
        places.append(jnp.sum(before * h, axis=0, keepdims=True))
        run = run + jnp.sum(h, axis=1, keepdims=True)
    return jnp.concatenate(places, axis=1), jnp.max(run)


def pack(parts, ids, weight, group, groups, room, write):
    lanes = ids.shape[1]
    valid = weight > 0.0
    hot = jnp.where((iota((groups, lanes), 0) == group) & valid, 1.0, 0.0)
    pos, most = place(hot)
    pos = pos.astype(I32)
    keep = valid & (pos < room - 1)
    slot = jnp.where(keep, group * room + pos, -1)
    pick = as_bf16(iota((groups * room, lanes), 0) == slot)
    out = chosen(pick, parts)
    w = weight.astype(I32)
    pieces = [
        shift_div(ids, 16384),
        shift_div(ids, 128) & 127,
        ids & 127,
        shift_div(w, 128),
        w & 127,
    ]
    row = iota((8, lanes), 0)
    stack = jnp.zeros((8, lanes), F32)
    for k, piece in enumerate(pieces):
        stack = jnp.where(row == k, piece.astype(F32), stack)
    tags = nt_dot(stack.astype(BF16), pick)
    tag_ids = tags[0:1] * 16384.0 + tags[1:2] * 128.0 + tags[2:3]
    tag_w = tags[3:4] * 128.0 + tags[4:5]
    for g in range(groups):
        span = slice(g * room, (g + 1) * room)
        write(g, out[span], tag_ids[:, span], tag_w[:, span])
    return most


def flag_row(flag):
    return jnp.where(iota((1, LANES), 1) == LANES - 1, jnp.full((1, LANES), 1.0, F32) * flag, 0.0)


def padded(row):
    width = row.shape[1]
    if width == LANES:
        return row
    return jnp.concatenate([row, jnp.zeros((1, LANES - width), F32)], axis=1)


def write_block(ref, at, room, rows, tag_ids, tag_w):
    ref[at + (slice(0, room), slice(None))] = rows
    last = slice(room - 1, room)
    ref[at + (last, slice(0, LANES))] = padded(tag_ids)
    ref[at + (last, slice(LANES, 2 * LANES))] = padded(tag_w)


def write_news(ref, at, room, flag, counts):
    last = slice(room - 1, room)
    lane = iota((1, LANES), 1)
    ids = ref[at + (last, slice(0, LANES))]
    ref[at + (last, slice(0, LANES))] = jnp.where(lane == LANES - 1, flag_row(flag), ids)
    ref[at + (last, slice(2 * LANES, 3 * LANES))] = counts


def above(most, room):
    return jnp.where(most > room - 1, 1.0, 0.0)


def split_device(device, sizes):
    _, n_gy, n_gz = sizes
    gz = device & (n_gz - 1)
    gy = shift_div(device, n_gz) & (n_gy - 1)
    gx = shift_div(device, n_gz * n_gy)
    return gy, gx * n_gz + gz


def offsets(ids, me, sizes):
    gy, plane = split_device(shift_div(ids, CL_DEV), sizes)
    my_gy, my_plane = split_device(me, sizes)
    return gy ^ my_gy, plane ^ my_plane


def prepare_kernel(sizes, rooms, my_ref, points_ref, assign_ref, index_ref, *outs):
    _, n_gy, _ = sizes
    a_refs, b_refs = outs[:n_gy], outs[n_gy:]
    count_pts = points_ref.shape[0]
    half = points_ref.shape[1] // 2
    ids = assign_ref[...]
    hot = as_bf16(iota((count_pts, count_pts), 0) == index_ref[...])
    weight = nt_dot(jnp.ones((8, count_pts), BF16), hot)[0:1]
    wide = jnp.concatenate([nn_dot(hot, jnp.ones((count_pts, LANES), BF16))] * (half // LANES), axis=1)
    along, across = offsets(ids, my_ref[0], sizes)
    counts = demand(ids, weight)
    for refs, room, group, columns in (
        (a_refs, rooms[0], along, slice(0, half)),
        (b_refs, rooms[1], across, slice(half, 2 * half)),
    ):
        most = pack(
            split(points_ref[:, columns] * wide), ids, weight, group, len(refs), room,
            lambda g, *v: write_block(refs[g], (), room, *v),
        )
        for ref in refs:
            write_news(ref, (), room, above(most, room), counts)


def demand(ids, weight):
    owner = shift_div(ids, CL_DEV)
    hot = as_bf16(iota((LANES, ids.shape[1]), 0) == owner)
    return nt_dot(jnp.where(jnp.broadcast_to(weight, (8, ids.shape[1])) > 0.0, 1.0, 0.0).astype(BF16), hot)[0:1]


def gathered(blocks):
    rows, ids, weight = [], [], []
    first, counts = jnp.zeros((1, LANES), F32), jnp.zeros((1, LANES), F32)
    for block in blocks:
        room = block.shape[0]
        rows.append(block)
        last = block[room - 1 : room]
        ids.append(last[:, :room])
        weight.append(last[:, LANES : LANES + room])
        first = jnp.maximum(first, last[:, :LANES])
        counts = counts + last[:, 2 * LANES : 3 * LANES]
    flag = jnp.max(jnp.where(iota((1, LANES), 1) == LANES - 1, first, 0.0))
    return (
        jnp.concatenate(rows, axis=0),
        jnp.concatenate(ids, axis=1).astype(I32),
        jnp.concatenate(weight, axis=1),
        flag,
        counts,
    )


def forward_kernel(sizes, room, to_plane, count_in, my_ref, *refs):
    outs = refs[count_in:]
    rows, ids, weight, flag, counts = gathered([r[...] for r in refs[:count_in]])
    along, across = offsets(ids, my_ref[0], sizes)
    pack(
        split(rows), ids, weight, across if to_plane else along, len(outs), room,
        lambda g, *v: write_block(outs[g], (), room, *v),
    )
    flag = jnp.maximum(flag, above(jnp.max(counts), room))
    for ref in outs:
        write_news(ref, (), room, flag, counts)


def finish_kernel(counts_in, my_ref, *refs):
    count_a, count_b = counts_in
    a_in, b_in = refs[:count_a], refs[count_a : count_a + count_b]
    means_ref, cent_ref, flag_ref, xa_ref, xb_ref, ta_ref, tb_ref = refs[count_a + count_b :]
    block = means_ref.shape[0]
    step = pl.program_id(0)

    @pl.when(step == 0)
    def _():
        flags = []
        for blocks, x_ref, t_ref in ((a_in, xa_ref, ta_ref), (b_in, xb_ref, tb_ref)):
            rows, ids, weight, flag, _ = gathered([r[...] for r in blocks])
            flags.append(flag)
            x_ref[...] = split(rows)
            t_ref[0:1, :] = jnp.where(weight > 0.0, ids - my_ref[0] * CL_DEV, -1)
            t_ref[1:2, :] = weight.astype(I32)
        flag_ref[0, 0] = jnp.where(jnp.maximum(flags[0], flags[1]) > 0.0, 1, 0)

    first = step * block
    sums = []
    for x_ref, t_ref in ((xa_ref, ta_ref), (xb_ref, tb_ref)):
        hot = as_bf16(iota((block, t_ref.shape[1]), 0) + first == t_ref[0:1, :])
        sums.append(chosen(hot, x_ref[...]))
    w = tb_ref[1:2, :]
    lanes = w.shape[1]
    high = jnp.broadcast_to(shift_div(w, 128).astype(F32), (LANES, lanes))
    low = jnp.broadcast_to((w & 127).astype(F32), (LANES, lanes))
    pair = nt_dot(hot, jnp.concatenate([high, low], axis=0).astype(BF16))
    share = 1.0 / jnp.maximum(pair[:, :LANES] * 128.0 + pair[:, LANES:], 1.0)
    left, right = [x * jnp.concatenate([share] * (x.shape[1] // LANES), axis=1) for x in sums]
    square = jnp.sum(left * left, axis=1, keepdims=True) + jnp.sum(right * right, axis=1, keepdims=True)
    scale = 1.0 / jnp.sqrt(square + 1e-06)
    width_a = left.shape[1]
    means_ref[:, :width_a] = left
    means_ref[:, width_a:] = right
    cent_ref[:, :width_a] = left * scale
    cent_ref[:, width_a:] = right * scale


VMEM_SPEC = pl.BlockSpec(memory_space=pltpu.VMEM)
SMEM_SPEC = pl.BlockSpec(memory_space=pltpu.SMEM)


def body(points, assignment, sample_index):
    count_pts, features = points.shape
    half = features // 2
    sizes = tuple(lax.axis_size(a) for a in ("gx", "gy", "gz"))
    n_gx, n_gy, n_gz = sizes
    n_plane = n_gx * n_gz
    devices = n_gx * n_gy * n_gz
    capacity = 2 * count_pts // devices

    def room(groups, slack, most):
        return min(8 * ((5 * count_pts // (8 * groups) + slack + 7) // 8), 8 * (most // 8 + 1), LANES)

    room_a1 = room(n_gy, count_pts // 16, n_plane * capacity)
    room_b1 = room(n_plane, count_pts // 16, n_gy * capacity)
    room_a2 = room(n_plane, count_pts * 5 // 64, n_gy * capacity)
    room_b2 = room(n_gy, count_pts * 3 // 32, n_plane * capacity)
    my_gx, my_gy, my_gz = (lax.axis_index(a) for a in ("gx", "gy", "gz"))
    me = ((my_gx * n_gy + my_gy) * n_gz + my_gz).astype(I32).reshape(1)

    def exchange(blocks, axes):
        out = [blocks[0]]
        for r in range(1, len(blocks)):
            out.append(lax.ppermute(blocks[r], axes, [(i, i ^ r) for i in range(len(blocks))]))
        return out

    def cost(us):
        return pl.CostEstimate(flops=us * 7_000_000, bytes_accessed=1 << 20, transcendentals=0)

    def vmem(mib, **others):
        return pltpu.CompilerParams(vmem_limit_bytes=mib << 20, **others)

    def shape(*dims):
        return jax.ShapeDtypeStruct(dims, F32)

    assign = assignment.reshape(1, count_pts)
    assign = assignment.reshape(1, count_pts)
    sent = pl.pallas_call(
        functools.partial(prepare_kernel, sizes, (room_a1, room_b1)),
        in_specs=[SMEM_SPEC] + [VMEM_SPEC] * 3,
        out_specs=[VMEM_SPEC] * (n_gy + n_plane),
        out_shape=[shape(room_a1, half)] * n_gy + [shape(room_b1, half)] * n_plane,
        compiler_params=vmem(12),
        cost_estimate=cost(5),
        name="prepare",
    )(me, points, assignment.reshape(1, count_pts), sample_index.reshape(1, count_pts))
    a1 = exchange(sent[:n_gy], "gy")
    b1 = exchange(sent[n_gy:], ("gx", "gz"))

    def forward(blocks, to_plane, room):
        count = n_plane if to_plane else n_gy
        return pl.pallas_call(
            functools.partial(forward_kernel, sizes, room, to_plane, len(blocks)),
            in_specs=[SMEM_SPEC] + [VMEM_SPEC] * len(blocks),
            out_specs=[VMEM_SPEC] * count,
            out_shape=[shape(room, half)] * count,
            compiler_params=vmem(8),
            cost_estimate=cost(3),
        )(me, *blocks)

    a2 = exchange(forward(a1, True, room_a2), ("gx", "gz"))
    b2 = exchange(forward(b1, False, room_b2), "gy")
    steps = 4
    block = CL_DEV // steps
    lanes_a, lanes_b = n_plane * room_a2, n_gy * room_b2
    means, centroids, over = pl.pallas_call(
        functools.partial(finish_kernel, (n_plane, n_gy)),
        grid=(steps,),
        in_specs=[SMEM_SPEC] + [VMEM_SPEC] * (n_plane + n_gy),
        out_specs=[pl.BlockSpec((block, features), lambda i: (i, 0))] * 2 + [SMEM_SPEC],
        out_shape=[shape(CL_DEV, features)] * 2 + [jax.ShapeDtypeStruct((1, 1), I32)],
        scratch_shapes=[
            pltpu.VMEM((lanes_a, PARTS * half), BF16),
            pltpu.VMEM((lanes_b, PARTS * half), BF16),
            pltpu.VMEM((8, lanes_a), I32),
            pltpu.VMEM((8, lanes_b), I32),
        ],
        compiler_params=vmem(18, dimension_semantics=("arbitrary",)),
        cost_estimate=cost(6),
        name="finish",
    )(me, *a2, *b2)

    def again(carry):
        return (jnp.int32(0),) + full_body(points, assignment, sample_index)

    return lax.while_loop(lambda carry: carry[0] > 0, again, (over[0, 0], means, centroids))[1:]


def solution(mesh):
    return jax.shard_map(
        body,
        mesh=mesh,
        in_specs=(P(("gx", "gy", "gz"), None), P(("gx", "gy", "gz")), P(("gx", "gy", "gz"))),
        out_specs=(P(("gx", "gy", "gz"), None), P(("gx", "gy", "gz"), None)),
        check_vma=False,
    )
```
